256 devices in a mesh: north: 8 (over x, core), east: 32 (over z, y).
Axes of the slice: x: 4, y: 4, z: 8, core: 2. Of those that a mesh axis runs over, the one named last changes fastest.
Arguments:
- left_factor: bfloat16 [8192, 8192], P('north', 'east'), may hold values from -6 to 6
- right_factor: bfloat16 [8192, 16384], P('north', 'east'), may hold values from -0.0625 to 0.0625
Outputs:
- updated: float32 [8192, 16384], P('north', 'east')
The draws below stay inside these ranges and needn't reach their ends.
All inputs are finite; a program needn't handle non-finite values.
Results may differ from the reference program's by a relative error of at most 0.0003.
Values may be sent and summed in bfloat16 or wider, within the bound.
A program may use at most 128 MiB of HBM per device.

```python
import jax
import jax.numpy as jnp
from jax import lax

ROWS = 8192
COLS = 16384
INNER = 8192


def block_levels(own_key, dims, cuts, smallest, top_value):
    def one(position, blocks):
        steps = jax.random.uniform(jax.random.fold_in(jax.random.fold_in(own_key, 6), position), (blocks,), jnp.float32, smallest / len(cuts), top_value / len(cuts))
        return jnp.repeat(jnp.exp(steps), dims[position] // blocks).reshape((-1,) + (1,) * (len(dims) - position - 1))

    gain = one(*cuts[0])
    for cut in cuts[1:]:
        gain = gain * one(*cut)
    return gain


def gaussian(own_key, extent, deviation, most, pieces=(), kind=jnp.bfloat16):
    result = jax.random.normal(own_key, extent, jnp.float32) * deviation
    if len(pieces) > 0:
        result = block_levels(own_key, extent, pieces, -0.22, 0.18) * result
    return jnp.clip(result, min=-most, max=most).astype(kind)


def setup_inputs(seed: int = 0) -> dict:
    streams_of = jax.random.split(jax.random.key(seed), 3)
    left_factor = gaussian(streams_of[0], (ROWS, INNER), 1.0, 6.0, ((0, 8), (1, 32)))
    right_factor = gaussian(streams_of[1], (INNER, COLS), INNER ** -0.5, 0.0625, ((0, 8), (1, 32)))
    return dict(left_factor=left_factor, right_factor=right_factor)


def reference(left_factor, right_factor):
    updated = jnp.dot(left_factor, right_factor, preferred_element_type=jnp.float32)
    row_power = lax.optimization_barrier(jnp.sum(updated * updated, axis=1))
    updated = updated * lax.rsqrt(row_power / COLS + 1e-06)[:, None]
    return updated
```

```python
import functools

import jax
import jax.numpy as jnp
from jax import lax
from jax.experimental import pallas as pl
from jax.experimental.pallas import tpu as pltpu
from jax.sharding import PartitionSpec as P

MESH = pl.DeviceIdType.MESH
LANES = 128
GROUPS = 4
TOP = 32768.0
TAIL = 16
LINK_RATE = 46.6e3
CORE_RATE = 600e3
LINK_LATENCY = 2.0
CORE_LATENCY = 1.0
WINDOW = 2.5
MULTIPLY = 0.5
FINISH = 0.6
UNITS = [(0, 0), (1, 1), (3, 0), (2, 0), (2, 1), (1, 0), (3, 1), (0, 1)]
USES = {
    ("dir", 0): (1, 1), ("dir", 1): (3, 0),
    ("two", 0): (2, 0), ("two", 1): (2, 1),
    ("acc", 0): (1, 0), ("acc", 1): (3, 1),
}
KINDS = ("two", "dir", "acc")


class Item:
    def __init__(self, key, deps, rank, emit, link=None, size=0, takes=0.0):
        self.key, self.deps, self.rank, self.emit = key, deps, rank, emit
        self.link, self.size, self.takes = link, size, takes


def plan(items):
    ready, free, order = {}, {}, []
    left = list(items)
    now = 0.0
    while left:
        best = None
        for item in left:
            if any(d not in ready for d in item.deps):
                continue
            at = max([ready[d] for d in item.deps], default=0.0)
            if item.link:
                at = max(at, free.get(item.link, 0.0) - WINDOW)
            at = max(at, now)
            trial = (at, 0 if item.link else 1, item.rank)
            if best is None or trial < best[0]:
                best = (trial, item)
        (at, _, _), item = best
        now = at
        if item.link:
            near = item.link == "core"
            begin = max(now, free.get(item.link, 0.0))
            free[item.link] = begin + item.size / (CORE_RATE if near else LINK_RATE)
            ready[item.key] = free[item.link] + (CORE_LATENCY if near else LINK_LATENCY)
            now += 0.03
        else:
            now += item.takes
            ready[item.key] = now
        order.append(item)
        left.remove(item)
    return order, ready


def kernel(
    xs, ys, zs, a_hbm, b_hbm, out, left, right, relay, code_out, code_in,
    sums_own, sums_in, load, sent, came, s_sent, s_came,
):
    rows, depth = a_hbm.shape
    columns = b_hbm.shape[1]
    n = ys * zs
    half = columns // 2
    group = rows // GROUPS
    chunk = group // 2

    me_north, me = lax.axis_index("north"), lax.axis_index("east")
    x, core = lax.div(me_north, 2), lax.rem(me_north, 2)
    z, y = lax.div(me, ys), lax.rem(me, ys)

    def turn(v, by, size):
        return lax.rem(v + (by + size), size)

    def x_at(by):
        return 2 * turn(x, by, xs) + core

    def y_at(by):
        return z * ys + turn(y, by, ys)

    def z_at(by):
        return turn(z, by, zs) * ys + y

    partner = (2 * x + 1 - core, me)
    toward = {
        "x0": (x_at(1), me), "x1": (x_at(-1), me),
        "y0": (me_north, y_at(1)), "y1": (me_north, y_at(-1)),
        "z0": (me_north, z_at(1)), "z1": (me_north, z_at(-1)),
        "core": partner,
    }

    def slab(north):
        return pl.ds(pl.multiple_of(north * depth, depth), depth)

    def cols(h):
        return pl.ds(h * half, half)

    own_left = left.at[:, slab(z)]
    load_a = pltpu.make_async_copy(a_hbm, own_left, load.at[0])
    load_b = pltpu.make_async_copy(b_hbm.at[slab(y)], right.at[0, slab(me_north)], load.at[1])
    load_a.start()
    load_b.start()

    barrier = pltpu.get_barrier_semaphore()
    for device in toward.values():
        pl.semaphore_signal(barrier, inc=1, device_id=device, device_id_type=MESH)
    pl.semaphore_wait(barrier, len(toward))

    items, copies, waits = [], {}, {("load", 0): load_a.wait, ("load", 1): load_b.wait}
    ready_at_start = [("load", 0), ("load", 1)]

    def send(key, deps, rank, link, source, target):
        i = len(copies)
        copy = pltpu.make_async_remote_copy(
            src_ref=source, dst_ref=target, send_sem=sent.at[i], recv_sem=came.at[i],
            device_id=toward[link], device_id_type=MESH,
        )
        copies[key] = copy
        waits[key] = copy.wait_recv
        size = 2 * source.shape[0] * source.shape[1]
        items.append(Item(key, deps, rank, copy.start, link, size))

    arrived = {p: [] for p in range(GROUPS)}
    for p in range(GROUPS):
        for s in range(2):
            here = pl.ds(p * group + s * chunk, chunk)
            for d in range(2):
                hops = zs // 2 - (s + d) % 2
                for h in range(hops):
                    block = left.at[here, slab(turn(z, h if d else -h, zs))]
                    key = ("a", p, s, d, h)
                    send(
                        key, [("a", p, s, d, h - 1)] if h else [], (p, h, s), f"z{d}",
                        block if h else a_hbm.at[here], block,
                    )
                    arrived[p].append(key)

    place = {u: i for i, u in enumerate(UNITS)}
    base = {}
    for d, j in ((0, 3), (1, 1)):
        block = b_hbm.at[slab(turn(y, -1 if d else 1, ys))]
        for h in range(2):
            base[j, h] = [("by", j, h)]
            send(
                ("by", j, h), [], (0, place[j, h]), f"y{d}",
                block.at[:, cols(h)], right.at[j, slab(me_north), cols(h)],
            )
    far = b_hbm.at[slab(turn(y, 2, ys))]
    for h in range(2):
        base[0, h], base[2, h] = [], [("by", 2, h)]
        send(("far", h), [], (0, place[2, h]), f"y{h}", far.at[:, cols(h)], relay.at[h])
        send(
            ("by", 2, h), [("far", h)], (0, place[2, h]), f"y{h}",
            relay.at[h], right.at[2, slab(me_north), cols(h)],
        )
    have = {}
    for u in UNITS:
        j, h = u
        rank = (0, place[u])
        mine = right.at[j, slab(me_north), cols(h)]
        source = mine if j else b_hbm.at[slab(y), cols(h)]
        landed = list(base[u]) if j else [("load", 1)]
        for d in range(2):
            send(("bx", u, d, 1), base[u], rank, f"x{d}", source, mine)
            landed.append(("bx", u, d, 1))
        passed = right.at[j, slab(x_at(1 if h else -1)), cols(h)]
        send(("bx", u, h, 2), [("bx", u, h, 1)], rank, f"x{h}", passed, passed)
        landed.append(("bx", u, h, 2))
        for t in range(xs):
            block = right.at[j, slab(x_at(-t)), cols(h)] if t else source
            target = right.at[j, slab(x_at(-t)), cols(h)]
            deps = [base[u], [("bx", u, 0, 1)], [("bx", u, h, 2)], [("bx", u, 1, 1)]][t]
            send(("bd", u, t), deps, rank, "core", block, target)
            landed.append(("bd", u, t))
        have[u] = landed

    def multiply(p, u):
        j, h = u
        return jnp.dot(
            left[p * group:(p + 1) * group, :], right[j, :, h * half:(h + 1) * half],
            preferred_element_type=jnp.float32,
        )

    def decode(p, k):
        coded = code_in[p, k, :group, :].astype(jnp.float32)
        scale = code_in[p, k, group:group + 1, :].astype(jnp.float32) * (1.0 / TOP)
        size = lax.rsqrt(lax.rsqrt(jnp.maximum(jnp.abs(coded), 1e-37)))
        size = size * lax.rsqrt(size)
        return jnp.where(coded < 0, -size, size) * scale

    def encode(p, k, value):
        most = jnp.maximum(jnp.max(jnp.abs(value), axis=0, keepdims=True), 1e-30)
        scale = most.astype(jnp.bfloat16)
        power = value * (TOP / scale.astype(jnp.float32))
        power = power * power
        power = power * power
        power = power * power
        code_out[p, k, :group, :] = jnp.where(value < 0, -power, power).astype(jnp.bfloat16)
        code_out[p, k, group:, :] = jnp.broadcast_to(scale, (TAIL, half))

    def slot(kind, d):
        return 2 * KINDS.index(kind) + d

    def part(p, kind, d):
        def run():
            value = multiply(p, USES[kind, d])
            if kind == "acc":
                value = value + decode(p, slot("two", d))
            encode(p, slot(kind, d), value)
        return run

    def own(p, h):
        def run():
            out[p * group:(p + 1) * group, h * half:(h + 1) * half] = multiply(p, (0, h))
        return run

    def finish(p):
        def run():
            here = slice(p * group, (p + 1) * group)
            narrow = None
            for h in range(2):
                value = out[here, h * half:(h + 1) * half]
                value = value + decode(p, slot("dir", 1 - h)) + decode(p, slot("acc", h))
                out[here, h * half:(h + 1) * half] = value
                value = value * value
                for k in range(0, half, LANES):
                    term = value[:, k:k + LANES]
                    narrow = term if narrow is None else narrow + term
            sums_own[:, here] = jnp.sum(narrow.T, axis=0, keepdims=True)
        return run

    for p in range(GROUPS):
        rows_in = arrived[p] + [("load", 0)]
        for k, kind in enumerate(KINDS):
            for d in range(2):
                deps = rows_in + have[USES[kind, d]]
                if kind == "acc":
                    deps = deps + [("c", p, "two", d)]
                items.append(Item(("k", p, kind, d), deps, (p, k, d), part(p, kind, d), takes=MULTIPLY))
                i = slot(kind, d)
                send(
                    ("c", p, kind, d), [("k", p, kind, d)], (1, p, k), f"y{d}",
                    code_out.at[p, i], code_in.at[p, i],
                )
        for h in range(2):
            items.append(Item(("own", p, h), rows_in + have[0, h], (p + GROUPS, 0, h), own(p, h), takes=MULTIPLY))
        deps = [("own", p, 0), ("own", p, 1)]
        deps += [("c", p, kind, d) for kind in ("dir", "acc") for d in range(2)]
        items.append(Item(("fin", p), deps, (p, 9, 0), finish(p), takes=FINISH))

    shares = ((0, (GROUPS - 1) * group), ((GROUPS - 1) * group, group))
    s_copies = [
        [
            pltpu.make_async_remote_copy(
                src_ref=sums_own.at[:, pl.ds(*share)], dst_ref=sums_in.at[k - 1, :, pl.ds(*share)],
                send_sem=s_sent.at[i, k - 1], recv_sem=s_came.at[i, k - 1],
                device_id=(me_north, lax.rem(me + k, n)), device_id_type=MESH,
            )
            for k in range(1, n)
        ]
        for i, share in enumerate(shares)
    ]

    def tell(i):
        def run():
            for copy in s_copies[i]:
                copy.start()
        return run

    items.append(Item(("s", 0), [("fin", p) for p in range(GROUPS - 1)], (GROUPS, 0), tell(0), takes=0.5))
    items.append(Item(("s", 1), [("fin", GROUPS - 1)], (GROUPS, 1), tell(1), takes=0.5))

    for key in ready_at_start:
        items.insert(0, Item(key, [], (-1,), lambda: None))
    order, _ = plan(items)
    waited = set()
    for item in order:
        for key in item.deps:
            if key in waits and key not in waited:
                waits[key]()
                waited.add(key)
        item.emit()
    for key in waits:
        if key not in waited:
            waits[key]()

    for group_copies in s_copies:
        for copy in group_copies:
            copy.wait_recv()
    total = sums_own[...]
    for k in range(n - 1):
        total = total + sums_in[k]
    scale = lax.rsqrt(total / (columns * n) + 1e-06)
    piece = 256
    for begin in range(0, rows, piece):
        gain = jnp.broadcast_to(scale[:, begin:begin + piece], (LANES, piece)).T
        for k in range(0, columns, LANES):
            out[pl.ds(begin, piece), k:k + LANES] *= gain
    for copy in copies.values():
        copy.wait_send()
    for group_copies in s_copies:
        for copy in group_copies:
            copy.wait_send()


def shards(xs, ys, zs, left, right):
    rows, depth = left.shape
    columns = right.shape[1]
    half = columns // 2
    group = rows // GROUPS
    peers = ys * zs - 1
    count = 14 * 2 * GROUPS // 2 * (zs // 8) + 8 + 8 * 7 + 6 * GROUPS
    dma = pltpu.SemaphoreType.DMA
    count = GROUPS * 2 * (zs - 1) + 8 + 7 * len(UNITS) + 6 * GROUPS
    return pl.pallas_call(
        functools.partial(kernel, xs, ys, zs),
        out_shape=jax.ShapeDtypeStruct((rows, columns), jnp.float32),
        in_specs=[pl.BlockSpec(memory_space=pl.ANY)] * 2,
        out_specs=pl.BlockSpec(memory_space=pltpu.VMEM),
        scratch_shapes=[
            pltpu.VMEM((rows, depth * zs), left.dtype),
            pltpu.VMEM((ys, depth * 2 * xs, columns), right.dtype),
            pltpu.VMEM((2, depth, half), right.dtype),
            pltpu.VMEM((GROUPS, 6, group + TAIL, half), jnp.bfloat16),
            pltpu.VMEM((GROUPS, 6, group + TAIL, half), jnp.bfloat16),
            pltpu.VMEM((1, rows), jnp.float32),
            pltpu.VMEM((peers, 1, rows), jnp.float32),
            dma((2,)),
            dma((count,)),
            dma((count,)),
            dma((2, peers)),
            dma((2, peers)),
        ],
        compiler_params=pltpu.CompilerParams(
            collective_id=0, has_side_effects=True, vmem_limit_bytes=56 << 20
        ),
    )(left, right)


def solution(mesh):
    xs = mesh.shape["north"] // 2
    ys = xs
    zs = mesh.shape["east"] // ys
    placed = (P("north", "east"), P("north", "east"))
    return jax.shard_map(
        functools.partial(shards, xs, ys, zs),
        mesh=mesh, in_specs=placed, out_specs=P("north", "east"), check_vma=False,
    )
```

```python
import functools

import jax
import jax.numpy as jnp
from jax import lax
from jax.experimental import pallas as pl
from jax.experimental.pallas import tpu as pltpu
from jax.sharding import PartitionSpec as P

MESH = pl.DeviceIdType.MESH
LANES = 128
GROUPS = (192, 192, 192, 192, 128, 128)
LATE = 4
EARLY = 2
TOP = 32768.0
TAIL = 8
HEAD = 16
LINK_RATE = 46.6e3
CORE_RATE = 600e3
LINK_LATENCY = 2.8
CORE_LATENCY = 1.0
FAR_SOURCE = 0.5
WINDOW = 2.5
SLACK = 0.0
PACE = 3
MULTIPLY = 0.7 / 256
CODE = 0.13 / 256
FINISH = 0.53 / 256
KINDS = ("two", "dir", "acc", "own")
FIRST = 1
USES = {
    "two": ((2, 0), (2, 1)), "dir": ((1, 1), (3, 0)),
    "acc": ((1, 0), (3, 1)), "own": ((0, 0), (0, 1)),
}
STEPS = {"two": 2, "dir": 2, "acc": 2, "own": 1}
TURN = {"dir": 0, "two": 1, "acc": 2, "own": 3}


class Item:
    def __init__(self, key, deps, rank, emit, link=None, size=0, takes=0.0, late=0.0):
        self.key, self.deps, self.rank, self.emit = key, deps, rank, emit
        self.link, self.size, self.takes, self.late = link, size, takes, late


def plan(items):
    ready, free, order = {}, {}, []
    left = list(items)
    now = 0.0
    while left:
        best = None
        able = [
            (item, max([ready[d] for d in item.deps], default=0.0))
            for item in left if all(d in ready for d in item.deps)
        ]
        for item, at in able:
            if item.link:
                at = max(at, free.get(item.link, 0.0) - WINDOW, now)
                until = max(free.get(item.link, 0.0), at) + SLACK
                for other, when in able:
                    sooner = other.link == item.link and other.rank[0] < item.rank[0] - 1
                    if sooner and at < when <= until:
                        at = when + 0.01
            trial = (max(at, now), 0 if item.link else 1, item.rank)
            if best is None or trial < best[0]:
                best = (trial, item)
        (now, _, _), item = best
        if item.link:
            near = item.link == "core"
            begin = max(now, free.get(item.link, 0.0))
            free[item.link] = begin + item.size / (CORE_RATE if near else LINK_RATE)
            ready[item.key] = free[item.link] + (CORE_LATENCY if near else LINK_LATENCY) + item.late
            now += 0.03
        else:
            now += item.takes
            ready[item.key] = now
        order.append(item)
        left.remove(item)
    return order, ready


def kernel(xs, ys, zs, a_hbm, b_hbm, out, left, right, relay, sums_own, *rest):
    parts = len(GROUPS)
    code_out, rest = rest[:parts], rest[parts:]
    code_in, rest = rest[:parts], rest[parts:]
    (peak, gain_out), rest = rest[:2], rest[2:]
    sums_in, rest = rest[:2], rest[2:]
    load, a_sent, b_sent, c_sent, s_sent, came, a_came, b_came, two_came, end_came, s_came = rest
    rows, depth = a_hbm.shape
    columns = b_hbm.shape[1]
    n = ys * zs
    half = columns // 2
    start = [sum(GROUPS[:p]) for p in range(parts)]
    inner = depth * zs

    me_north, me = lax.axis_index("north"), lax.axis_index("east")
    x, core = lax.div(me_north, 2), lax.rem(me_north, 2)
    z, y = lax.div(me, ys), lax.rem(me, ys)

    def turn(v, by, size):
        return lax.rem(v + (by + size), size)

    def x_at(by):
        return 2 * turn(x, by, xs) + core

    def y_at(by):
        return z * ys + turn(y, by, ys)

    def z_at(by):
        return turn(z, by, zs) * ys + y

    partner = (2 * x + 1 - core, me)
    toward = {
        "x0": (x_at(1), me), "x1": (x_at(-1), me),
        "y0": (me_north, y_at(1)), "y1": (me_north, y_at(-1)),
        "z0": (me_north, z_at(1)), "z1": (me_north, z_at(-1)),
        "core": partner,
    }

    def slab(north):
        return pl.ds(pl.multiple_of(north * depth, depth), depth)

    def width(kind):
        return half // STEPS[kind]

    def cols(kind, d, b):
        return pl.ds(USES[kind][d][1] * half + b * width(kind), width(kind))

    def right_piece(kind, d, b, north):
        return right.at[
            KINDS.index(kind), slab(north), pl.ds((2 * b + d) * width(kind), width(kind))
        ]

    load_a = pltpu.make_async_copy(a_hbm, left.at[pl.ds(HEAD, rows), slab(z)], load.at[0])
    load_b = pltpu.make_async_copy(
        b_hbm.at[slab(y)], right.at[KINDS.index("own"), slab(me_north)], load.at[1]
    )
    load_a.start()
    load_b.start()

    barrier = pltpu.get_barrier_semaphore()
    for device in toward.values():
        pl.semaphore_signal(barrier, inc=1, device_id=device, device_id_type=MESH)
    load_a.wait()
    largest = jnp.max(jnp.abs(left[pl.ds(HEAD, rows), slab(z)].astype(jnp.float32)), axis=0, keepdims=True)
    largest = jnp.broadcast_to(jnp.max(largest, axis=1, keepdims=True), (HEAD, depth))
    left[pl.ds(0, HEAD), slab(z)] = largest.astype(left.dtype)
    pl.semaphore_wait(barrier, len(toward))

    def whole(ref, sem):
        return pltpu.make_async_remote_copy(
            src_ref=ref, dst_ref=ref, send_sem=sem, recv_sem=sem,
            device_id=partner, device_id_type=MESH,
        )

    items = []
    waits = {("load", 1): load_b.wait}
    for key in list(waits):
        items.append(Item(key, [], (-1.0,), lambda: None))
    single = []

    def send(key, deps, rank, link, source, target, sent, arrives=None, late=0.0):
        if arrives is None:
            arrives = came.at[len(single)]
            single.append(key)
        copy = pltpu.make_async_remote_copy(
            src_ref=source, dst_ref=target, send_sem=sent, recv_sem=arrives,
            device_id=toward[link], device_id_type=MESH,
        )
        if single and single[-1] == key:
            waits[key] = copy.wait_recv
        size = 2 * source.shape[0] * source.shape[1]
        items.append(Item(key, deps, (rank,), copy.start, link, size, late=late))

    arrived = []
    for p in range(parts):
        chunk = GROUPS[p] // 2
        last = []
        for s in range(2):
            head = HEAD if p + s == 0 else 0
            here = pl.ds(HEAD - head + start[p] + s * chunk, head + chunk)
            source = pl.ds(start[p] + s * chunk, chunk)
            for d in range(2):
                hops = zs // 2 - (s + d) % 2
                for h in range(hops):
                    block = left.at[here, slab(turn(z, h if d else -h, zs))]
                    key = ("a", p, s, d, h)
                    send(
                        key, [("a", p, s, d, h - 1)] if h else [], PACE * min(p, parts - 2) + h + 0.01 * s, f"z{d}",
                        block if h or head else a_hbm.at[source], block, a_sent.at[0],
                        a_came.at[p] if h == hops - 1 else None, 0 if h else FAR_SOURCE,
                    )
                last.append(key)
        key = ("a", p)
        items.append(Item(key, last, (-1.0,), lambda: None))
        size = left.at[pl.ds(0, 4 * chunk + (0 if p else 2 * HEAD)), pl.ds(0, depth)]
        waits[key] = whole(size, a_came.at[p]).wait_recv
        arrived.append([key])

    have = {}
    for i, kind in enumerate(KINDS):
        for b in range(STEPS[kind]):
            rank = 3 * TURN[kind] + 1.5 * b
            have[kind, b] = [("b", kind, b)] + ([("load", 1)] if kind == "own" else [])
            near = []
            for d, (j, h) in enumerate(USES[kind]):
                u = (kind, d, b)
                mine = right_piece(*u, me_north)
                base = [("by", u)] if j else []
                if j:
                    target = b_hbm.at[slab(turn(y, -j, ys)), cols(*u)]
                    link = f"y{h}" if j == 2 else ("y0" if j == 3 else "y1")
                    if j == 2:
                        send(
                            ("far", u), [], rank, link, target, relay.at[h, b], b_sent.at[0],
                            late=FAR_SOURCE,
                        )
                        send(("by", u), [("far", u)], rank, link, relay.at[h, b], mine, b_sent.at[0])
                    else:
                        send(("by", u), [], rank, link, target, mine, b_sent.at[0], late=FAR_SOURCE)
                source = mine if j else b_hbm.at[slab(y), cols(*u)]
                for e in range(2):
                    send(
                        ("bx", u, e, 1), base, rank + (0.0 if e == h else 0.1), f"x{e}",
                        source, mine, b_sent.at[0], late=0 if j else FAR_SOURCE,
                    )
                passed = right_piece(*u, x_at(1 if h else -1))
                send(
                    ("bx", u, h, 2), [("bx", u, h, 1)], rank - 1, f"x{h}",
                    passed, passed, b_sent.at[0],
                )
                have[kind, b] += base + [("bx", u, 0, 1), ("bx", u, 1, 1), ("bx", u, h, 2)]
                for t in range(xs):
                    place = right_piece(*u, x_at(-t))
                    deps = [base, [("bx", u, 0, 1)], [("bx", u, h, 2)], [("bx", u, 1, 1)]][t]
                    send(
                        ("bd", u, t), deps, rank, "core", place if t else source, place,
                        b_sent.at[0], b_came.at[2 * i + b],
                    )
                    near.append(("bd", u, t))
            items.append(Item(("b", kind, b), near, (-1.0,), lambda: None))
            size = right.at[i, pl.ds(0, depth * xs), pl.ds(0, 2 * width(kind))]
            waits["b", kind, b] = whole(size, b_came.at[2 * i + b]).wait_recv

    def multiply(p, kind, b=None):
        across = slice(None) if b is None else slice(b * half, (b + 1) * half)
        return jnp.dot(
            left[HEAD + start[p]:HEAD + start[p] + GROUPS[p], :], right[KINDS.index(kind), :, across],
            preferred_element_type=jnp.float32,
        )

    def scale_in(k, across):
        return code_in[0][k, GROUPS[0]:GROUPS[0] + 1, across].astype(jnp.float32)

    def decode(p, k, across):
        coded = code_in[p][k, :GROUPS[p], across].astype(jnp.float32)
        size = lax.rsqrt(lax.rsqrt(jnp.maximum(jnp.abs(coded), 1e-37)))
        size = size * lax.rsqrt(size)
        return jnp.where(coded < 0, -size, size) * (scale_in(k, across) * (1.0 / TOP))

    def encode(p, k, across, value):
        power = value * gain_out[k, :, across]
        power = power * power
        power = power * power
        power = power * power
        code_out[p][k, :GROUPS[p], across] = jnp.where(value < 0, -power, power).astype(jnp.bfloat16)

    def set_scale(kind, b):
        i = KINDS.index(kind)
        if kind == KINDS[FIRST]:
            if b == 0:
                most = jnp.max(left[:HEAD, :].astype(jnp.float32), axis=0, keepdims=True)
                peak[...] = jnp.broadcast_to(jnp.max(most, axis=1, keepdims=True) * inner, peak.shape)
        for d in range(2):
            first = (2 * b + d) * width(kind)
            across = slice(b * width(kind), (b + 1) * width(kind))
            block = right[i, :, first:first + width(kind)]
            bound = jnp.max(jnp.abs(block.astype(jnp.float32)), axis=0, keepdims=True) * peak[...]
            if kind == "acc":
                bound = bound + scale_in(slot("two", d), across)
            scale = jnp.maximum(bound, 1e-30).astype(jnp.bfloat16)
            gain_out[slot(kind, d), :, across] = TOP / scale.astype(jnp.float32)
            code_out[0][slot(kind, d), GROUPS[0]:, across] = jnp.broadcast_to(scale, (TAIL, width(kind)))

    def slot(kind, d):
        return 2 * KINDS.index(kind) + d

    def part(p, kind, b):
        def run():
            if p == 0:
                set_scale(kind, b)
            value = multiply(p, kind, b)
            for c in range(STEPS[kind]) if b is None else (b,):
                across = slice(c * width(kind), (c + 1) * width(kind))
                for d in range(2):
                    first = (2 * (c if b is None else 0) + d) * width(kind)
                    block = value[:, first:first + width(kind)]
                    if kind == "acc":
                        block = block + decode(p, slot("two", d), across)
                    encode(p, slot(kind, d), across, block)
        return run

    def own(p):
        def run():
            out[start[p]:start[p] + GROUPS[p], :] = multiply(p, "own")
        return run

    def finish(p):
        def run():
            here = slice(start[p], start[p] + GROUPS[p])
            narrow = None
            for h in range(2):
                value = out[here, h * half:(h + 1) * half]
                value = value + decode(p, slot("dir", 1 - h), slice(None)) + decode(p, slot("acc", h), slice(None))
                out[here, h * half:(h + 1) * half] = value
                value = value * value
                for k in range(0, half, LANES):
                    term = value[:, k:k + LANES]
                    narrow = term if narrow is None else narrow + term
            sums_own[:, here] = jnp.sum(narrow.T, axis=0, keepdims=True)
        return run

    for p in range(parts):
        sent_rows = pl.ds(0, GROUPS[p] + (0 if p else TAIL))
        ends = []
        for k, kind in enumerate(KINDS[:3]):
            split = STEPS[kind] == 2 and p < EARLY
            for b in range(2) if split else (None,):
                deps = list(arrived[p])
                for c in range(STEPS[kind]) if b is None else (b,):
                    deps += have[kind, c]
                c = b or 0
                if kind == "acc":
                    deps.append(("two", p, c))
                if p:
                    deps += [("k", 0, kind, e) for e in range(2)]
                if kind != KINDS[FIRST]:
                    deps.append(("k", 0, KINDS[FIRST], 0))
                rank = 3 * p + 4 * k + 0.1 * c
                takes = (MULTIPLY * (0.95 if split else 1.0) + CODE * (0.5 if split else 1.0)) * GROUPS[p] + (0 if p else 0.2)
                items.append(Item(("k", p, kind, c), deps, (rank,), part(p, kind, b), takes=takes))
                across = pl.ds(c * half // 2, half // 2) if split else pl.ds(0, half)
                for d in range(2):
                    i = slot(kind, d)
                    send(
                        ("c", p, kind, c, d), [("k", p, kind, c)], rank, f"y{d}",
                        code_out[p].at[i, sent_rows, across], code_in[p].at[i, sent_rows, across], c_sent.at[p],
                        two_came.at[2 * p + c] if kind == "two" else end_came.at[p],
                    )
                sent = [("c", p, kind, c, d) for d in range(2)]
                if kind == "two":
                    items.append(Item(("two", p, c), sent, (-1.0,), lambda: None))
                    size = code_in[p].at[pl.ds(0, 2), sent_rows, across]
                    waits["two", p, c] = whole(size, two_came.at[2 * p + c]).wait_recv
                else:
                    ends += sent
        deps = arrived[p] + have["own", 0]
        items.append(Item(("own", p), deps, (1000 + p,), own(p), takes=MULTIPLY * GROUPS[p]))
        items.append(Item(("end", p), ends, (-1.0,), lambda: None))
        waits["end", p] = whole(code_in[p].at[pl.ds(2, 4), sent_rows], end_came.at[p]).wait_recv
        deps = [("own", p), ("end", p), ("end", 0)]
        items.append(Item(("fin", p), deps, (500 + p,), finish(p), takes=FINISH * GROUPS[p]))

    shares = ((0, start[LATE]), (start[LATE], rows - start[LATE]))

    def tell(i):
        def run():
            for k in range(1, n):
                pltpu.make_async_remote_copy(
                    src_ref=sums_own.at[:, pl.ds(*shares[i])], dst_ref=sums_in[i].at[k - 1],
                    send_sem=s_sent.at[i], recv_sem=s_came.at[i],
                    device_id=(me_north, lax.rem(me + k, n)), device_id_type=MESH,
                ).start()
        return run

    early = [("fin", p) for p in range(LATE)]
    items.append(Item(("s", 0), early, (2000,), tell(0), takes=0.3))
    late = [("fin", p) for p in range(LATE, parts)]
    items.append(Item(("s", 1), late + [("s", 0)], (2001,), tell(1), takes=0.3))

    order, _ = plan(items)
    waited = set()
    for item in order:
        for key in item.deps:
            if key in waits and key not in waited:
                waits[key]()
                waited.add(key)
        item.emit()

    piece = 128
    for i, (begin, count) in enumerate(shares):
        whole(sums_in[i], s_came.at[i]).wait_recv()
        total = sums_own[:, pl.ds(begin, count)]
        for k in range(n - 1):
            total = total + sums_in[i][k]
        scale = lax.rsqrt(total / (columns * n) + 1e-06)
        for r in range(0, count, piece):
            gain = jnp.broadcast_to(scale[:, r:r + piece], (LANES, piece)).T
            for k in range(0, columns, LANES):
                out[pl.ds(begin + r, piece), k:k + LANES] *= gain
    whole(left.at[:, pl.ds(0, depth * (zs - 1))], a_sent.at[0]).wait_send()
    whole(right, b_sent.at[0]).wait_send()
    for p in range(parts):
        whole(code_out[p], c_sent.at[p]).wait_send()
    for i in range(2):
        whole(sums_in[i], s_sent.at[i]).wait_send()


def shards(xs, ys, zs, left, right):
    rows, depth = left.shape
    columns = right.shape[1]
    half = columns // 2
    parts = len(GROUPS)
    peers = ys * zs - 1
    dma = pltpu.SemaphoreType.DMA
    codes = [pltpu.VMEM((6, group + (0 if p else TAIL), half), jnp.bfloat16) for p, group in enumerate(GROUPS)]
    pieces = sum(2 * STEPS[kind] for kind in KINDS)
    single = parts * (2 * (zs - 1) - 4) + 3 * pieces + sum(2 * STEPS[kind] for kind in KINDS[:3]) + 2 * STEPS["two"]
    factors = [pltpu.with_memory_space_constraint(v, pltpu.HBM) for v in (left, right)]
    return pl.pallas_call(
        functools.partial(kernel, xs, ys, zs),
        out_shape=jax.ShapeDtypeStruct((rows, columns), jnp.float32),
        in_specs=[pl.BlockSpec(memory_space=pltpu.HBM)] * 2,
        out_specs=pl.BlockSpec(memory_space=pltpu.VMEM),
        scratch_shapes=[
            pltpu.VMEM((HEAD + rows, depth * zs), left.dtype),
            pltpu.VMEM((len(KINDS), depth * 2 * xs, columns), right.dtype),
            pltpu.VMEM((2, STEPS["two"], depth, half // STEPS["two"]), right.dtype),
            pltpu.VMEM((1, rows), jnp.float32),
            *codes,
            *codes,
            pltpu.VMEM((1, half // 2), jnp.float32),
            pltpu.VMEM((6, 1, half), jnp.float32),
            pltpu.VMEM((peers, 1, sum(GROUPS[:LATE])), jnp.float32),
            pltpu.VMEM((peers, 1, sum(GROUPS[LATE:])), jnp.float32),
            dma((2,)),
            dma((1,)),
            dma((1,)),
            dma((parts,)),
            dma((2,)),
            dma((single,)),
            dma((parts,)),
            dma((2 * len(KINDS),)),
            dma((2 * parts,)),
            dma((parts,)),
            dma((2,)),
        ],
        compiler_params=pltpu.CompilerParams(
            collective_id=0, has_side_effects=True, vmem_limit_bytes=40 << 20
        ),
    )(*factors)


def solution(mesh):
    xs = mesh.shape["north"] // 2
    ys = xs
    zs = mesh.shape["east"] // ys
    placed = (P("north", "east"), P("north", "east"))
    return jax.shard_map(
        functools.partial(shards, xs, ys, zs),
        mesh=mesh, in_specs=placed, out_specs=P("north", "east"), check_vma=False,
    )
```

```python
import functools

import jax
import jax.numpy as jnp
from jax import lax
from jax.experimental import pallas as pl
from jax.experimental.pallas import tpu as pltpu
from jax.sharding import PartitionSpec as P

MESH = pl.DeviceIdType.MESH
LANES = 128
GROUPS = (192, 192, 192, 192, 128, 128)
LATE = 4
EARLY = 2
TOP = 32768.0
TAIL = 8
HEAD = 16
LINK_RATE = 45e3
CORE_RATE = 600e3
LINK_LATENCY = 2.8
CORE_LATENCY = 1.0
FAR_SOURCE = 0.5
WINDOW = 3.5
SLACK = 0.0
PACE = 3
MULTIPLY = 0.7 / 256
CODE = 0.13 / 256
FINISH = 0.53 / 256
KINDS = ("two", "dir", "acc", "own")
FIRST = 1
USES = {
    "two": ((2, 0), (2, 1)), "dir": ((1, 1), (3, 0)),
    "acc": ((1, 0), (3, 1)), "own": ((0, 0), (0, 1)),
}
STEPS = {"two": 2, "dir": 2, "acc": 2, "own": 1}
TURN = {"dir": 0, "two": 1, "acc": 2, "own": 3}


class Item:
    def __init__(self, key, deps, rank, emit, link=None, size=0, takes=0.0, late=0.0):
        self.key, self.deps, self.rank, self.emit = key, deps, rank, emit
        self.link, self.size, self.takes, self.late = link, size, takes, late


def plan(items):
    ready, free, order = {}, {}, []
    left = list(items)
    now = 0.0
    while left:
        best = None
        able = [
            (item, max([ready[d] for d in item.deps], default=0.0))
            for item in left if all(d in ready for d in item.deps)
        ]
        for item, at in able:
            if item.link:
                at = max(at, free.get(item.link, 0.0) - WINDOW, now)
                until = max(free.get(item.link, 0.0), at) + SLACK
                for other, when in able:
                    sooner = other.link == item.link and other.rank[0] < item.rank[0] - 1
                    if sooner and at < when <= until:
                        at = when + 0.01
            trial = (max(at, now), 0 if item.link else 1, item.rank)
            if best is None or trial < best[0]:
                best = (trial, item)
        (now, _, _), item = best
        if item.link:
            near = item.link == "core"
            begin = max(now, free.get(item.link, 0.0))
            free[item.link] = begin + item.size / (CORE_RATE if near else LINK_RATE)
            ready[item.key] = free[item.link] + (CORE_LATENCY if near else LINK_LATENCY) + item.late
            now += 0.03
        else:
            now += item.takes
            ready[item.key] = now
        order.append(item)
        left.remove(item)
    return order, ready


def kernel(xs, ys, zs, a_hbm, b_hbm, out, left, right, relay, sums_own, *rest):
    parts = len(GROUPS)
    code_out, rest = rest[:parts], rest[parts:]
    code_in, rest = rest[:parts], rest[parts:]
    (peak, gain_out), rest = rest[:2], rest[2:]
    sums_in, rest = rest[:2], rest[2:]
    load, a_sent, b_sent, c_sent, s_sent, came, a_came, b_came, two_came, end_came, s_came = rest
    rows, depth = a_hbm.shape
    columns = b_hbm.shape[1]
    n = ys * zs
    half = columns // 2
    start = [sum(GROUPS[:p]) for p in range(parts)]
    inner = depth * zs

    me_north, me = lax.axis_index("north"), lax.axis_index("east")
    x, core = lax.div(me_north, 2), lax.rem(me_north, 2)
    z, y = lax.div(me, ys), lax.rem(me, ys)

    def turn(v, by, size):
        return lax.rem(v + (by + size), size)

    def x_at(by):
        return 2 * turn(x, by, xs) + core

    def y_at(by):
        return z * ys + turn(y, by, ys)

    def z_at(by):
        return turn(z, by, zs) * ys + y

    partner = (2 * x + 1 - core, me)
    toward = {
        "x0": (x_at(1), me), "x1": (x_at(-1), me),
        "y0": (me_north, y_at(1)), "y1": (me_north, y_at(-1)),
        "z0": (me_north, z_at(1)), "z1": (me_north, z_at(-1)),
        "core": partner,
    }

    def slab(north):
        return pl.ds(pl.multiple_of(north * depth, depth), depth)

    def width(kind):
        return half // STEPS[kind]

    def cols(kind, d, b):
        return pl.ds(USES[kind][d][1] * half + b * width(kind), width(kind))

    def right_piece(kind, d, b, north):
        return right.at[
            KINDS.index(kind), slab(north), pl.ds((2 * b + d) * width(kind), width(kind))
        ]

    load_a = pltpu.make_async_copy(a_hbm, left.at[pl.ds(HEAD, rows), slab(z)], load.at[0])
    load_b = pltpu.make_async_copy(
        b_hbm.at[slab(y)], right.at[KINDS.index("own"), slab(me_north)], load.at[1]
    )
    load_a.start()
    load_b.start()

    barrier = pltpu.get_barrier_semaphore()
    for device in toward.values():
        pl.semaphore_signal(barrier, inc=1, device_id=device, device_id_type=MESH)
    pl.semaphore_wait(barrier, len(toward))

    def set_head():
        part = left[pl.ds(HEAD, rows), slab(z)].astype(jnp.float32)
        most = jnp.max(jnp.abs(part), axis=0, keepdims=True)
        most = jnp.broadcast_to(jnp.max(most, axis=1, keepdims=True), (HEAD, depth))
        left[pl.ds(0, HEAD), slab(z)] = most.astype(left.dtype)

    def whole(ref, sem):
        return pltpu.make_async_remote_copy(
            src_ref=ref, dst_ref=ref, send_sem=sem, recv_sem=sem,
            device_id=partner, device_id_type=MESH,
        )

    items = []
    waits = {("load", 0): load_a.wait, ("load", 1): load_b.wait}
    for key in list(waits):
        items.append(Item(key, [], (-1.0,), lambda: None))
    items.append(Item(("head",), [("load", 0)], (-0.5,), set_head, takes=0.3))
    single = []

    def send(key, deps, rank, link, source, target, sent, arrives=None, late=0.0):
        if arrives is None:
            arrives = came.at[len(single)]
            single.append(key)
        copy = pltpu.make_async_remote_copy(
            src_ref=source, dst_ref=target, send_sem=sent, recv_sem=arrives,
            device_id=toward[link], device_id_type=MESH,
        )
        if single and single[-1] == key:
            waits[key] = copy.wait_recv
        size = 2 * source.shape[0] * source.shape[1]
        items.append(Item(key, deps, (rank,), copy.start, link, size, late=late))

    arrived = []
    for p in range(parts):
        chunk = GROUPS[p] // 2
        last = []
        for s in range(2):
            head = HEAD if p == 0 and s == 1 else 0
            begin = start[p] + (s if p else 1 - s) * chunk
            here = pl.ds(HEAD - head + begin, head + chunk)
            source = pl.ds(begin, chunk)
            for d in range(2):
                hops = zs // 2 - (s + d) % 2
                for h in range(hops):
                    block = left.at[here, slab(turn(z, h if d else -h, zs))]
                    key = ("a", p, s, d, h)
                    send(
                        key, [("a", p, s, d, h - 1)] if h else [("head",)] if head else [], PACE * min(p, parts - 2) + h + 0.01 * s, f"z{d}",
                        block if h or head else a_hbm.at[source], block, a_sent.at[0],
                        a_came.at[p] if h == hops - 1 else None, 0 if h else FAR_SOURCE,
                    )
                last.append(key)
        key = ("a", p)
        items.append(Item(key, last, (-1.0,), lambda: None))
        size = left.at[pl.ds(0, 4 * chunk + (0 if p else 2 * HEAD)), pl.ds(0, depth)]
        waits[key] = whole(size, a_came.at[p]).wait_recv
        arrived.append([key])

    have = {}
    for i, kind in enumerate(KINDS):
        for b in range(STEPS[kind]):
            rank = 3 * TURN[kind] + 1.5 * b
            have[kind, b] = [("b", kind, b)] + ([("load", 1)] if kind == "own" else [])
            near = []
            for d, (j, h) in enumerate(USES[kind]):
                u = (kind, d, b)
                mine = right_piece(*u, me_north)
                base = [("by", u)] if j else []
                if j:
                    target = b_hbm.at[slab(turn(y, -j, ys)), cols(*u)]
                    link = f"y{h}" if j == 2 else ("y0" if j == 3 else "y1")
                    if j == 2:
                        send(
                            ("far", u), [], rank, link, target, relay.at[h, b], b_sent.at[0],
                            late=FAR_SOURCE,
                        )
                        send(("by", u), [("far", u)], rank, link, relay.at[h, b], mine, b_sent.at[0])
                    else:
                        send(("by", u), [], rank, link, target, mine, b_sent.at[0], late=FAR_SOURCE)
                source = mine if j else b_hbm.at[slab(y), cols(*u)]
                for e in range(2):
                    send(
                        ("bx", u, e, 1), base, rank + (0.0 if e == h else 0.1), f"x{e}",
                        source, mine, b_sent.at[0], late=0 if j else FAR_SOURCE,
                    )
                passed = right_piece(*u, x_at(1 if h else -1))
                send(
                    ("bx", u, h, 2), [("bx", u, h, 1)], rank - 1, f"x{h}",
                    passed, passed, b_sent.at[0],
                )
                have[kind, b] += base + [("bx", u, 0, 1), ("bx", u, 1, 1), ("bx", u, h, 2)]
                for t in range(xs):
                    place = right_piece(*u, x_at(-t))
                    deps = [base, [("bx", u, 0, 1)], [("bx", u, h, 2)], [("bx", u, 1, 1)]][t]
                    send(
                        ("bd", u, t), deps, rank, "core", place if t else source, place,
                        b_sent.at[0], b_came.at[2 * i + b],
                    )
                    near.append(("bd", u, t))
            items.append(Item(("b", kind, b), near, (-1.0,), lambda: None))
            size = right.at[i, pl.ds(0, depth * xs), pl.ds(0, 2 * width(kind))]
            waits["b", kind, b] = whole(size, b_came.at[2 * i + b]).wait_recv

    def multiply(p, kind, b=None):
        across = slice(None) if b is None else slice(b * half, (b + 1) * half)
        return jnp.dot(
            left[HEAD + start[p]:HEAD + start[p] + GROUPS[p], :], right[KINDS.index(kind), :, across],
            preferred_element_type=jnp.float32,
        )

    def scale_in(k, across):
        return code_in[0][k, GROUPS[0]:GROUPS[0] + 1, across].astype(jnp.float32)

    def decode(p, k, across):
        coded = code_in[p][k, :GROUPS[p], across].astype(jnp.float32)
        size = lax.rsqrt(lax.rsqrt(jnp.maximum(jnp.abs(coded), 1e-37)))
        size = size * lax.rsqrt(size)
        return jnp.where(coded < 0, -size, size) * (scale_in(k, across) * (1.0 / TOP))

    def encode(p, k, across, value):
        power = value * gain_out[k, :, across]
        power = power * power
        power = power * power
        power = power * power
        code_out[p][k, :GROUPS[p], across] = jnp.where(value < 0, -power, power).astype(jnp.bfloat16)

    def set_scale(kind, b):
        i = KINDS.index(kind)
        if kind == KINDS[FIRST]:
            if b == 0:
                most = jnp.max(left[:HEAD, :].astype(jnp.float32), axis=0, keepdims=True)
                peak[...] = jnp.broadcast_to(jnp.max(most, axis=1, keepdims=True) * inner, peak.shape)
        for d in range(2):
            first = (2 * b + d) * width(kind)
            across = slice(b * width(kind), (b + 1) * width(kind))
            block = right[i, :, first:first + width(kind)]
            bound = jnp.max(jnp.abs(block.astype(jnp.float32)), axis=0, keepdims=True) * peak[...]
            if kind == "acc":
                bound = bound + scale_in(slot("two", d), across)
            scale = jnp.maximum(bound, 1e-30).astype(jnp.bfloat16)
            gain_out[slot(kind, d), :, across] = TOP / scale.astype(jnp.float32)
            code_out[0][slot(kind, d), GROUPS[0]:, across] = jnp.broadcast_to(scale, (TAIL, width(kind)))

    def slot(kind, d):
        return 2 * KINDS.index(kind) + d

    def part(p, kind, b):
        def run():
            if p == 0:
                set_scale(kind, b)
            value = multiply(p, kind, b)
            for c in range(STEPS[kind]) if b is None else (b,):
                across = slice(c * width(kind), (c + 1) * width(kind))
                for d in range(2):
                    first = (2 * (c if b is None else 0) + d) * width(kind)
                    block = value[:, first:first + width(kind)]
                    if kind == "acc":
                        block = block + decode(p, slot("two", d), across)
                    encode(p, slot(kind, d), across, block)
        return run

    def own(p):
        def run():
            out[start[p]:start[p] + GROUPS[p], :] = multiply(p, "own")
        return run

    def finish(p):
        def run():
            here = slice(start[p], start[p] + GROUPS[p])
            narrow = None
            for h in range(2):
                value = out[here, h * half:(h + 1) * half]
                value = value + decode(p, slot("dir", 1 - h), slice(None)) + decode(p, slot("acc", h), slice(None))
                out[here, h * half:(h + 1) * half] = value
                value = value * value
                for k in range(0, half, LANES):
                    term = value[:, k:k + LANES]
                    narrow = term if narrow is None else narrow + term
            sums_own[:, here] = jnp.sum(narrow.T, axis=0, keepdims=True)
        return run

    for p in range(parts):
        sent_rows = pl.ds(0, GROUPS[p] + (0 if p else TAIL))
        ends = []
        for k, kind in enumerate(KINDS[:3]):
            split = STEPS[kind] == 2 and p < EARLY
            for b in range(2) if split else (None,):
                deps = list(arrived[p])
                for c in range(STEPS[kind]) if b is None else (b,):
                    deps += have[kind, c]
                c = b or 0
                if kind == "acc":
                    deps.append(("two", p, c))
                if p:
                    deps += [("k", 0, kind, e) for e in range(2)]
                if kind != KINDS[FIRST]:
                    deps.append(("k", 0, KINDS[FIRST], 0))
                rank = 3 * p + 4 * k + 0.1 * c
                takes = (MULTIPLY * (0.95 if split else 1.0) + CODE * (0.5 if split else 1.0)) * GROUPS[p] + (0 if p else 0.2)
                items.append(Item(("k", p, kind, c), deps, (rank,), part(p, kind, b), takes=takes))
                across = pl.ds(c * half // 2, half // 2) if split else pl.ds(0, half)
                for d in range(2):
                    i = slot(kind, d)
                    send(
                        ("c", p, kind, c, d), [("k", p, kind, c)], rank, f"y{d}",
                        code_out[p].at[i, sent_rows, across], code_in[p].at[i, sent_rows, across], c_sent.at[p],
                        two_came.at[2 * p + c] if kind == "two" else end_came.at[p],
                    )
                sent = [("c", p, kind, c, d) for d in range(2)]
                if kind == "two":
                    items.append(Item(("two", p, c), sent, (-1.0,), lambda: None))
                    size = code_in[p].at[pl.ds(0, 2), sent_rows, across]
                    waits["two", p, c] = whole(size, two_came.at[2 * p + c]).wait_recv
                else:
                    ends += sent
        deps = arrived[p] + have["own", 0]
        items.append(Item(("own", p), deps, (1000 + p,), own(p), takes=MULTIPLY * GROUPS[p]))
        items.append(Item(("end", p), ends, (-1.0,), lambda: None))
        waits["end", p] = whole(code_in[p].at[pl.ds(2, 4), sent_rows], end_came.at[p]).wait_recv
        deps = [("own", p), ("end", p), ("end", 0)]
        items.append(Item(("fin", p), deps, (500 + p,), finish(p), takes=FINISH * GROUPS[p]))

    shares = ((0, start[LATE]), (start[LATE], rows - start[LATE]))

    def tell(i):
        def run():
            for k in range(1, n):
                pltpu.make_async_remote_copy(
                    src_ref=sums_own.at[:, pl.ds(*shares[i])], dst_ref=sums_in[i].at[k - 1],
                    send_sem=s_sent.at[i], recv_sem=s_came.at[i],
                    device_id=(me_north, lax.rem(me + k, n)), device_id_type=MESH,
                ).start()
        return run

    early = [("fin", p) for p in range(LATE)]
    items.append(Item(("s", 0), early, (2000,), tell(0), takes=0.3))
    late = [("fin", p) for p in range(LATE, parts)]
    items.append(Item(("s", 1), late + [("s", 0)], (2001,), tell(1), takes=0.3))

    order, _ = plan(items)
    waited = set()
    for item in order:
        for key in item.deps:
            if key in waits and key not in waited:
                waits[key]()
                waited.add(key)
        item.emit()

    piece = 128
    for i, (begin, count) in enumerate(shares):
        whole(sums_in[i], s_came.at[i]).wait_recv()
        total = sums_own[:, pl.ds(begin, count)]
        for k in range(n - 1):
            total = total + sums_in[i][k]
        scale = lax.rsqrt(total / (columns * n) + 1e-06)
        for r in range(0, count, piece):
            gain = jnp.broadcast_to(scale[:, r:r + piece], (LANES, piece)).T
            for k in range(0, columns, LANES):
                out[pl.ds(begin + r, piece), k:k + LANES] *= gain
    whole(left.at[:, pl.ds(0, depth * (zs - 1))], a_sent.at[0]).wait_send()
    whole(right, b_sent.at[0]).wait_send()
    for p in range(parts):
        whole(code_out[p], c_sent.at[p]).wait_send()
    for i in range(2):
        whole(sums_in[i], s_sent.at[i]).wait_send()


def shards(xs, ys, zs, left, right):
    rows, depth = left.shape
    columns = right.shape[1]
    half = columns // 2
    parts = len(GROUPS)
    peers = ys * zs - 1
    dma = pltpu.SemaphoreType.DMA
    codes = [pltpu.VMEM((6, group + (0 if p else TAIL), half), jnp.bfloat16) for p, group in enumerate(GROUPS)]
    pieces = sum(2 * STEPS[kind] for kind in KINDS)
    single = parts * (2 * (zs - 1) - 4) + 3 * pieces + sum(2 * STEPS[kind] for kind in KINDS[:3]) + 2 * STEPS["two"]
    factors = [pltpu.with_memory_space_constraint(v, pltpu.HBM) for v in (left, right)]
    return pl.pallas_call(
        functools.partial(kernel, xs, ys, zs),
        out_shape=jax.ShapeDtypeStruct((rows, columns), jnp.float32),
        in_specs=[pl.BlockSpec(memory_space=pltpu.HBM)] * 2,
        out_specs=pl.BlockSpec(memory_space=pltpu.VMEM),
        scratch_shapes=[
            pltpu.VMEM((HEAD + rows, depth * zs), left.dtype),
            pltpu.VMEM((len(KINDS), depth * 2 * xs, columns), right.dtype),
            pltpu.VMEM((2, STEPS["two"], depth, half // STEPS["two"]), right.dtype),
            pltpu.VMEM((1, rows), jnp.float32),
            *codes,
            *codes,
            pltpu.VMEM((1, half // 2), jnp.float32),
            pltpu.VMEM((6, 1, half), jnp.float32),
            pltpu.VMEM((peers, 1, sum(GROUPS[:LATE])), jnp.float32),
            pltpu.VMEM((peers, 1, sum(GROUPS[LATE:])), jnp.float32),
            dma((2,)),
            dma((1,)),
            dma((1,)),
            dma((parts,)),
            dma((2,)),
            dma((single,)),
            dma((parts,)),
            dma((2 * len(KINDS),)),
            dma((2 * parts,)),
            dma((parts,)),
            dma((2,)),
        ],
        compiler_params=pltpu.CompilerParams(
            collective_id=0, has_side_effects=True, vmem_limit_bytes=40 << 20
        ),
    )(*factors)


def solution(mesh):
    xs = mesh.shape["north"] // 2
    ys = xs
    zs = mesh.shape["east"] // ys
    placed = (P("north", "east"), P("north", "east"))
    return jax.shard_map(
        functools.partial(shards, xs, ys, zs),
        mesh=mesh, in_specs=placed, out_specs=P("north", "east"), check_vma=False,
    )
```

```python
import functools

import jax
import jax.numpy as jnp
from jax import lax
from jax.experimental import pallas as pl
from jax.experimental.pallas import tpu as pltpu
from jax.sharding import PartitionSpec as P

MESH = pl.DeviceIdType.MESH
LANES = 128
GROUPS = (192, 192, 192, 192, 128, 128)
LATE = 4
EARLY = 2
TOP = 32768.0
TAIL = 8
HEAD = 16
LINK_RATE = 45e3
CORE_RATE = 600e3
LINK_LATENCY = 2.8
CORE_LATENCY = 1.0
FAR_SOURCE = 0.5
WINDOW = 3.5
SLACK = 0.0
PACE = 3
MULTIPLY = 0.7 / 256
CODE = 0.13 / 256
FINISH = 0.53 / 256
KINDS = ("two", "dir", "acc", "own")
FIRST = 1
USES = {
    "two": ((2, 0), (2, 1)), "dir": ((1, 1), (3, 0)),
    "acc": ((1, 0), (3, 1)), "own": ((0, 0), (0, 1)),
}
STEPS = {"two": 2, "dir": 2, "acc": 2, "own": 1}
TURN = {"dir": 0, "two": 1, "acc": 2, "own": 3}


class Item:
    def __init__(self, key, deps, rank, emit, link=None, size=0, takes=0.0, late=0.0):
        self.key, self.deps, self.rank, self.emit = key, deps, rank, emit
        self.link, self.size, self.takes, self.late = link, size, takes, late


def plan(items):
    ready, free, order = {}, {}, []
    left = list(items)
    now = 0.0
    while left:
        best = None
        able = [
            (item, max([ready[d] for d in item.deps], default=0.0))
            for item in left if all(d in ready for d in item.deps)
        ]
        for item, at in able:
            if item.link:
                at = max(at, free.get(item.link, 0.0) - WINDOW, now)
                until = max(free.get(item.link, 0.0), at) + SLACK
                for other, when in able:
                    sooner = other.link == item.link and other.rank[0] < item.rank[0] - 1
                    if sooner and at < when <= until:
                        at = when + 0.01
            trial = (max(at, now), 0 if item.link else 1, item.rank)
            if best is None or trial < best[0]:
                best = (trial, item)
        (now, _, _), item = best
        if item.link:
            near = item.link == "core"
            begin = max(now, free.get(item.link, 0.0))
            free[item.link] = begin + item.size / (CORE_RATE if near else LINK_RATE)
            ready[item.key] = free[item.link] + (CORE_LATENCY if near else LINK_LATENCY) + item.late
            now += 0.03
        else:
            now += item.takes
            ready[item.key] = now
        order.append(item)
        left.remove(item)
    return order, ready


def kernel(xs, ys, zs, a_hbm, b_hbm, out, left, right, relay, sums_own, *rest):
    parts = len(GROUPS)
    code_out, rest = rest[:parts], rest[parts:]
    code_in, rest = rest[:parts], rest[parts:]
    (peak, gain_out), rest = rest[:2], rest[2:]
    sums_in, rest = rest[:2], rest[2:]
    load, a_sent, b_sent, c_sent, s_sent, came, a_came, b_came, two_came, end_came, s_came = rest
    rows, depth = a_hbm.shape
    columns = b_hbm.shape[1]
    n = ys * zs
    half = columns // 2
    start = [sum(GROUPS[:p]) for p in range(parts)]
    inner = depth * zs

    me_north, me = lax.axis_index("north"), lax.axis_index("east")
    x, core = lax.div(me_north, 2), lax.rem(me_north, 2)
    z, y = lax.div(me, ys), lax.rem(me, ys)

    def turn(v, by, size):
        return lax.rem(v + (by + size), size)

    def x_at(by):
        return 2 * turn(x, by, xs) + core

    def y_at(by):
        return z * ys + turn(y, by, ys)

    def z_at(by):
        return turn(z, by, zs) * ys + y

    partner = (2 * x + 1 - core, me)
    toward = {
        "x0": (x_at(1), me), "x1": (x_at(-1), me),
        "y0": (me_north, y_at(1)), "y1": (me_north, y_at(-1)),
        "z0": (me_north, z_at(1)), "z1": (me_north, z_at(-1)),
        "core": partner,
    }

    def slab(north):
        return pl.ds(pl.multiple_of(north * depth, depth), depth)

    def width(kind):
        return half // STEPS[kind]

    def cols(kind, d, b):
        return pl.ds(USES[kind][d][1] * half + b * width(kind), width(kind))

    def right_piece(kind, d, b, north):
        return right.at[
            KINDS.index(kind), slab(north), pl.ds((2 * b + d) * width(kind), width(kind))
        ]

    load_a = pltpu.make_async_copy(a_hbm, left.at[pl.ds(HEAD, rows), slab(z)], load.at[0])
    load_b = pltpu.make_async_copy(
        b_hbm.at[slab(y)], right.at[KINDS.index("own"), slab(me_north)], load.at[1]
    )
    load_a.start()
    load_b.start()

    barrier = pltpu.get_barrier_semaphore()
    for device in toward.values():
        pl.semaphore_signal(barrier, inc=1, device_id=device, device_id_type=MESH)
    pl.semaphore_wait(barrier, len(toward))

    def set_head():
        part = left[pl.ds(HEAD, rows), slab(z)].astype(jnp.float32)
        most = jnp.max(jnp.abs(part), axis=0, keepdims=True)
        most = jnp.broadcast_to(jnp.max(most, axis=1, keepdims=True), (HEAD, depth))
        left[pl.ds(0, HEAD), slab(z)] = most.astype(left.dtype)

    def whole(ref, sem):
        return pltpu.make_async_remote_copy(
            src_ref=ref, dst_ref=ref, send_sem=sem, recv_sem=sem,
            device_id=partner, device_id_type=MESH,
        )

    items = []
    waits = {("load", 0): load_a.wait, ("load", 1): load_b.wait}
    for key in list(waits):
        items.append(Item(key, [], (-1.0,), lambda: None))
    items.append(Item(("head",), [("load", 0)], (-0.5,), set_head, takes=0.3))
    single = []

    def send(key, deps, rank, link, source, target, sent, arrives=None, late=0.0):
        if arrives is None:
            arrives = came.at[len(single)]
            single.append(key)
        copy = pltpu.make_async_remote_copy(
            src_ref=source, dst_ref=target, send_sem=sent, recv_sem=arrives,
            device_id=toward[link], device_id_type=MESH,
        )
        if single and single[-1] == key:
            waits[key] = copy.wait_recv
        size = 2 * source.shape[0] * source.shape[1]
        items.append(Item(key, deps, (rank,), copy.start, link, size, late=late))

    arrived = []
    for p in range(parts):
        chunk = GROUPS[p] // 2
        last = []
        for s in range(2):
            head = HEAD if p == 0 and s == 1 else 0
            begin = start[p] + (s if p else 1 - s) * chunk
            here = pl.ds(HEAD - head + begin, head + chunk)
            source = pl.ds(begin, chunk)
            for d in range(2):
                hops = zs // 2 - (s + d) % 2
                for h in range(hops):
                    block = left.at[here, slab(turn(z, h if d else -h, zs))]
                    key = ("a", p, s, d, h)
                    send(
                        key, [("a", p, s, d, h - 1)] if h else [("head",)] if head else [], PACE * min(p, parts - 2) + h + 0.01 * s, f"z{d}",
                        block if h or head else a_hbm.at[source], block, a_sent.at[0],
                        a_came.at[p] if h == hops - 1 else None, 0 if h else FAR_SOURCE,
                    )
                last.append(key)
        key = ("a", p)
        items.append(Item(key, last, (-1.0,), lambda: None))
        size = left.at[pl.ds(0, 4 * chunk + (0 if p else 2 * HEAD)), pl.ds(0, depth)]
        waits[key] = whole(size, a_came.at[p]).wait_recv
        arrived.append([key])

    have = {}
    for i, kind in enumerate(KINDS):
        for b in range(STEPS[kind]):
            rank = 3 * TURN[kind] + 1.5 * b
            have[kind, b] = [("b", kind, b)] + ([("load", 1)] if kind == "own" else [])
            near = []
            for d, (j, h) in enumerate(USES[kind]):
                u = (kind, d, b)
                mine = right_piece(*u, me_north)
                base = [("by", u)] if j else []
                if j:
                    target = b_hbm.at[slab(turn(y, -j, ys)), cols(*u)]
                    link = f"y{h}" if j == 2 else ("y0" if j == 3 else "y1")
                    if j == 2:
                        send(
                            ("far", u), [], rank, link, target, relay.at[h, b], b_sent.at[0],
                            late=FAR_SOURCE,
                        )
                        send(("by", u), [("far", u)], rank, link, relay.at[h, b], mine, b_sent.at[0])
                    else:
                        send(("by", u), [], rank, link, target, mine, b_sent.at[0], late=FAR_SOURCE)
                source = mine if j else b_hbm.at[slab(y), cols(*u)]
                for e in range(2):
                    send(
                        ("bx", u, e, 1), base, rank + (0.0 if e == h else 0.1), f"x{e}",
                        source, mine, b_sent.at[0], late=0 if j else FAR_SOURCE,
                    )
                passed = right_piece(*u, x_at(1 if h else -1))
                send(
                    ("bx", u, h, 2), [("bx", u, h, 1)], rank - 1, f"x{h}",
                    passed, passed, b_sent.at[0],
                )
                have[kind, b] += base + [("bx", u, 0, 1), ("bx", u, 1, 1), ("bx", u, h, 2)]
                for t in range(xs):
                    place = right_piece(*u, x_at(-t))
                    deps = [base, [("bx", u, 0, 1)], [("bx", u, h, 2)], [("bx", u, 1, 1)]][t]
                    send(
                        ("bd", u, t), deps, rank, "core", place if t else source, place,
                        b_sent.at[0], b_came.at[2 * i + b],
                    )
                    near.append(("bd", u, t))
            items.append(Item(("b", kind, b), near, (-1.0,), lambda: None))
            size = right.at[i, pl.ds(0, depth * xs), pl.ds(0, 2 * width(kind))]
            waits["b", kind, b] = whole(size, b_came.at[2 * i + b]).wait_recv

    def multiply(p, kind, b=None):
        across = slice(None) if b is None else slice(b * half, (b + 1) * half)
        return jnp.dot(
            left[HEAD + start[p]:HEAD + start[p] + GROUPS[p], :], right[KINDS.index(kind), :, across],
            preferred_element_type=jnp.float32,
        )

    def scale_in(k, across):
        return code_in[0][k, GROUPS[0]:GROUPS[0] + 1, across].astype(jnp.float32)

    def decode(p, k, across):
        coded = code_in[p][k, :GROUPS[p], across].astype(jnp.float32)
        size = lax.rsqrt(lax.rsqrt(jnp.maximum(jnp.abs(coded), 1e-37)))
        size = size * lax.rsqrt(size)
        return jnp.where(coded < 0, -size, size) * (scale_in(k, across) * (1.0 / TOP))

    def encode(p, k, across, value):
        power = value * gain_out[k, :, across]
        power = power * power
        power = power * power
        power = power * power
        code_out[p][k, :GROUPS[p], across] = jnp.where(value < 0, -power, power).astype(jnp.bfloat16)

    def set_scale(kind, b):
        i = KINDS.index(kind)
        if kind == KINDS[FIRST]:
            if b == 0:
                most = jnp.max(left[:HEAD, :].astype(jnp.float32), axis=0, keepdims=True)
                peak[...] = jnp.broadcast_to(jnp.max(most, axis=1, keepdims=True) * inner, peak.shape)
        for d in range(2):
            first = (2 * b + d) * width(kind)
            across = slice(b * width(kind), (b + 1) * width(kind))
            block = right[i, :, first:first + width(kind)]
            bound = jnp.max(jnp.abs(block.astype(jnp.float32)), axis=0, keepdims=True) * peak[...]
            if kind == "acc":
                bound = bound + scale_in(slot("two", d), across)
            scale = jnp.maximum(bound, 1e-30).astype(jnp.bfloat16)
            gain_out[slot(kind, d), :, across] = TOP / scale.astype(jnp.float32)
            code_out[0][slot(kind, d), GROUPS[0]:, across] = jnp.broadcast_to(scale, (TAIL, width(kind)))

    def slot(kind, d):
        return 2 * KINDS.index(kind) + d

    def part(p, kind, b):
        def run():
            if p == 0:
                set_scale(kind, b)
            value = multiply(p, kind, b)
            for c in range(STEPS[kind]) if b is None else (b,):
                across = slice(c * width(kind), (c + 1) * width(kind))
                for d in range(2):
                    first = (2 * (c if b is None else 0) + d) * width(kind)
                    block = value[:, first:first + width(kind)]
                    if kind == "acc":
                        block = block + decode(p, slot("two", d), across)
                    encode(p, slot(kind, d), across, block)
        return run

    def own(p):
        def run():
            out[start[p]:start[p] + GROUPS[p], :] = multiply(p, "own")
        return run

    def finish(p):
        def run():
            here = slice(start[p], start[p] + GROUPS[p])
            narrow = None
            for h in range(2):
                value = out[here, h * half:(h + 1) * half]
                value = value + decode(p, slot("dir", 1 - h), slice(None)) + decode(p, slot("acc", h), slice(None))
                out[here, h * half:(h + 1) * half] = value
                value = value * value
                for k in range(0, half, LANES):
                    term = value[:, k:k + LANES]
                    narrow = term if narrow is None else narrow + term
            sums_own[:, here] = jnp.sum(narrow.T, axis=0, keepdims=True)
        return run

    def turn_of(p, c):
        return 2 * p + c if p < EARLY else EARLY + p

    for p in range(parts):
        sent_rows = pl.ds(0, GROUPS[p] + (0 if p else TAIL))
        ends = []
        for k, kind in enumerate(KINDS[:3]):
            split = STEPS[kind] == 2 and p < EARLY
            for b in range(2) if split else (None,):
                deps = list(arrived[p])
                for c in range(STEPS[kind]) if b is None else (b,):
                    deps += have[kind, c]
                c = b or 0
                if kind == "acc":
                    deps.append(("two", p, c))
                if p:
                    deps += [("k", 0, kind, e) for e in range(2)]
                if kind != KINDS[FIRST]:
                    deps.append(("k", 0, KINDS[FIRST], 0))
                rank = 3 * p + 4 * k + 0.1 * c
                takes = (MULTIPLY * (0.95 if split else 1.0) + CODE * (0.5 if split else 1.0)) * GROUPS[p] + (0 if p else 0.2)
                items.append(Item(("k", p, kind, c), deps, (rank,), part(p, kind, b), takes=takes))
                across = pl.ds(c * half // 2, half // 2) if split else pl.ds(0, half)
                for d in range(2):
                    i = slot(kind, d)
                    send(
                        ("c", p, kind, c, d), [("k", p, kind, c)], rank, f"y{d}",
                        code_out[p].at[i, sent_rows, across], code_in[p].at[i, sent_rows, across], c_sent.at[p],
                        two_came.at[turn_of(p, c)] if kind == "two" else end_came.at[p],
                    )
                sent = [("c", p, kind, c, d) for d in range(2)]
                if kind == "two":
                    items.append(Item(("two", p, c), sent, (-1.0,), lambda: None))
                    size = code_in[p].at[pl.ds(0, 2), sent_rows, across]
                    waits["two", p, c] = whole(size, two_came.at[turn_of(p, c)]).wait_recv
                else:
                    ends += sent
        deps = arrived[p] + have["own", 0]
        items.append(Item(("own", p), deps, (1000 + p,), own(p), takes=MULTIPLY * GROUPS[p]))
        items.append(Item(("end", p), ends, (-1.0,), lambda: None))
        waits["end", p] = whole(code_in[p].at[pl.ds(2, 4), sent_rows], end_came.at[p]).wait_recv
        deps = [("own", p), ("end", p), ("end", 0)]
        items.append(Item(("fin", p), deps, (500 + p,), finish(p), takes=FINISH * GROUPS[p]))

    shares = ((0, start[LATE]), (start[LATE], rows - start[LATE]))

    farthest = sorted(range(1, n), key=lambda k: abs(k - n // 2))

    def tell(i):
        def run():
            for k in farthest:
                pltpu.make_async_remote_copy(
                    src_ref=sums_own.at[:, pl.ds(*shares[i])], dst_ref=sums_in[i].at[k - 1],
                    send_sem=s_sent.at[i], recv_sem=s_came.at[i],
                    device_id=(me_north, lax.rem(me + k, n)), device_id_type=MESH,
                ).start()
        return run

    early = [("fin", p) for p in range(LATE)]
    items.append(Item(("s", 0), early, (2000,), tell(0), takes=0.3))
    late = [("fin", p) for p in range(LATE, parts)]
    items.append(Item(("s", 1), late + [("s", 0)], (2001,), tell(1), takes=0.3))

    order, _ = plan(items)
    waited = set()
    for item in order:
        for key in item.deps:
            if key in waits and key not in waited:
                waits[key]()
                waited.add(key)
        item.emit()

    piece = 128
    for i, (begin, count) in enumerate(shares):
        whole(sums_in[i], s_came.at[i]).wait_recv()
        total = sums_own[:, pl.ds(begin, count)]
        for k in range(n - 1):
            total = total + sums_in[i][k]
        scale = lax.rsqrt(total / (columns * n) + 1e-06)
        for r in range(0, count, piece):
            gain = jnp.broadcast_to(scale[:, r:r + piece], (LANES, piece)).T
            for k in range(0, columns, LANES):
                out[pl.ds(begin + r, piece), k:k + LANES] *= gain
    whole(left.at[:, pl.ds(0, depth * (zs - 1))], a_sent.at[0]).wait_send()
    whole(right, b_sent.at[0]).wait_send()
    for p in range(parts):
        whole(code_out[p], c_sent.at[p]).wait_send()
    for i in range(2):
        whole(sums_in[i], s_sent.at[i]).wait_send()


def shards(xs, ys, zs, left, right):
    rows, depth = left.shape
    columns = right.shape[1]
    half = columns // 2
    parts = len(GROUPS)
    peers = ys * zs - 1
    dma = pltpu.SemaphoreType.DMA
    codes = [pltpu.VMEM((6, group + (0 if p else TAIL), half), jnp.bfloat16) for p, group in enumerate(GROUPS)]
    pieces = sum(2 * STEPS[kind] for kind in KINDS)
    single = parts * (2 * (zs - 1) - 4) + 3 * pieces + sum(2 * STEPS[kind] for kind in KINDS[:3]) + 2 * STEPS["two"]
    factors = [pltpu.with_memory_space_constraint(v, pltpu.HBM) for v in (left, right)]
    return pl.pallas_call(
        functools.partial(kernel, xs, ys, zs),
        out_shape=jax.ShapeDtypeStruct((rows, columns), jnp.float32),
        in_specs=[pl.BlockSpec(memory_space=pltpu.HBM)] * 2,
        out_specs=pl.BlockSpec(memory_space=pltpu.VMEM),
        scratch_shapes=[
            pltpu.VMEM((HEAD + rows, depth * zs), left.dtype),
            pltpu.VMEM((len(KINDS), depth * 2 * xs, columns), right.dtype),
            pltpu.VMEM((2, STEPS["two"], depth, half // STEPS["two"]), right.dtype),
            pltpu.VMEM((1, rows), jnp.float32),
            *codes,
            *codes,
            pltpu.VMEM((1, half // 2), jnp.float32),
            pltpu.VMEM((6, 1, half), jnp.float32),
            pltpu.VMEM((peers, 1, sum(GROUPS[:LATE])), jnp.float32),
            pltpu.VMEM((peers, 1, sum(GROUPS[LATE:])), jnp.float32),
            dma((2,)),
            dma((1,)),
            dma((1,)),
            dma((parts,)),
            dma((2,)),
            dma((single,)),
            dma((parts,)),
            dma((2 * len(KINDS) - 1,)),
            dma((EARLY + parts,)),
            dma((parts,)),
            dma((2,)),
        ],
        compiler_params=pltpu.CompilerParams(
            collective_id=0, has_side_effects=True, vmem_limit_bytes=40 << 20
        ),
    )(*factors)


def solution(mesh):
    xs = mesh.shape["north"] // 2
    ys = xs
    zs = mesh.shape["east"] // ys
    placed = (P("north", "east"), P("north", "east"))
    return jax.shard_map(
        functools.partial(shards, xs, ys, zs),
        mesh=mesh, in_specs=placed, out_specs=P("north", "east"), check_vma=False,
    )
```

```python
import functools

import jax
import jax.numpy as jnp
from jax import lax
from jax.experimental import pallas as pl
from jax.experimental.pallas import tpu as pltpu
from jax.sharding import PartitionSpec as P

MESH = pl.DeviceIdType.MESH
LANES = 128
GROUPS = (192, 192, 192, 192, 128, 128)
LATE = 4
EARLY = 2
TOP = 32768.0
TAIL = 8
HEAD = 16
LINK_RATE = 45e3
CORE_RATE = 600e3
LINK_LATENCY = 2.8
CORE_LATENCY = 1.0
FAR_SOURCE = 0.5
WINDOW = 3.8
SLACK = 0.0
PACE = 3
MULTIPLY = 0.7 / 256
CODE = 0.13 / 256
FINISH = 0.53 / 256
KINDS = ("two", "dir", "acc", "own")
FIRST = 1
USES = {
    "two": ((2, 0), (2, 1)), "dir": ((1, 1), (3, 0)),
    "acc": ((1, 0), (3, 1)), "own": ((0, 0), (0, 1)),
}
STEPS = {"two": 2, "dir": 2, "acc": 2, "own": 1}
TURN = {"dir": 0, "two": 1, "acc": 2, "own": 3}


class Item:
    def __init__(self, key, deps, rank, emit, link=None, size=0, takes=0.0, late=0.0):
        self.key, self.deps, self.rank, self.emit = key, deps, rank, emit
        self.link, self.size, self.takes, self.late = link, size, takes, late


def plan(items):
    ready, free, order = {}, {}, []
    left = list(items)
    now = 0.0
    while left:
        best = None
        able = [
            (item, max([ready[d] for d in item.deps], default=0.0))
            for item in left if all(d in ready for d in item.deps)
        ]
        for item, at in able:
            if item.link:
                at = max(at, free.get(item.link, 0.0) - WINDOW, now)
                until = max(free.get(item.link, 0.0), at) + SLACK
                for other, when in able:
                    sooner = other.link == item.link and other.rank[0] < item.rank[0] - 1
                    if sooner and at < when <= until:
                        at = when + 0.01
            trial = (max(at, now), 0 if item.link else 1, item.rank)
            if best is None or trial < best[0]:
                best = (trial, item)
        (now, _, _), item = best
        if item.link:
            near = item.link == "core"
            begin = max(now, free.get(item.link, 0.0))
            free[item.link] = begin + item.size / (CORE_RATE if near else LINK_RATE)
            ready[item.key] = free[item.link] + (CORE_LATENCY if near else LINK_LATENCY) + item.late
            now += 0.03
        else:
            now += item.takes
            ready[item.key] = now
        order.append(item)
        left.remove(item)
    return order, ready


def kernel(xs, ys, zs, a_hbm, b_hbm, out, left, right, relay, sums_own, *rest):
    parts = len(GROUPS)
    code_out, rest = rest[:parts], rest[parts:]
    code_in, rest = rest[:parts], rest[parts:]
    (peak, gain_out), rest = rest[:2], rest[2:]
    sums_in, rest = rest[:2], rest[2:]
    load, a_sent, b_sent, c_sent, s_sent, came, a_came, b_came, two_came, end_came, s_came = rest
    rows, depth = a_hbm.shape
    columns = b_hbm.shape[1]
    n = ys * zs
    half = columns // 2
    start = [sum(GROUPS[:p]) for p in range(parts)]
    inner = depth * zs

    me_north, me = lax.axis_index("north"), lax.axis_index("east")
    x, core = lax.div(me_north, 2), lax.rem(me_north, 2)
    z, y = lax.div(me, ys), lax.rem(me, ys)

    def turn(v, by, size):
        return lax.rem(v + (by + size), size)

    def x_at(by):
        return 2 * turn(x, by, xs) + core

    def y_at(by):
        return z * ys + turn(y, by, ys)

    def z_at(by):
        return turn(z, by, zs) * ys + y

    partner = (2 * x + 1 - core, me)
    toward = {
        "x0": (x_at(1), me), "x1": (x_at(-1), me),
        "y0": (me_north, y_at(1)), "y1": (me_north, y_at(-1)),
        "z0": (me_north, z_at(1)), "z1": (me_north, z_at(-1)),
        "core": partner,
    }

    def slab(north):
        return pl.ds(pl.multiple_of(north * depth, depth), depth)

    def width(kind):
        return half // STEPS[kind]

    def cols(kind, d, b):
        return pl.ds(USES[kind][d][1] * half + b * width(kind), width(kind))

    def right_piece(kind, d, b, north):
        return right.at[
            KINDS.index(kind), slab(north), pl.ds((2 * b + d) * width(kind), width(kind))
        ]

    load_a = pltpu.make_async_copy(a_hbm, left.at[pl.ds(HEAD, rows), slab(z)], load.at[0])
    load_b = pltpu.make_async_copy(
        b_hbm.at[slab(y)], right.at[KINDS.index("own"), slab(me_north)], load.at[1]
    )
    load_a.start()
    load_b.start()

    barrier = pltpu.get_barrier_semaphore()
    for device in toward.values():
        pl.semaphore_signal(barrier, inc=1, device_id=device, device_id_type=MESH)
    pl.semaphore_wait(barrier, len(toward))

    def set_head():
        part = left[pl.ds(HEAD, rows), slab(z)].astype(jnp.float32)
        most = jnp.max(jnp.abs(part), axis=0, keepdims=True)
        most = jnp.broadcast_to(jnp.max(most, axis=1, keepdims=True), (HEAD, depth))
        left[pl.ds(0, HEAD), slab(z)] = most.astype(left.dtype)

    def whole(ref, sem):
        return pltpu.make_async_remote_copy(
            src_ref=ref, dst_ref=ref, send_sem=sem, recv_sem=sem,
            device_id=partner, device_id_type=MESH,
        )

    items = []
    waits = {("load", 0): load_a.wait, ("load", 1): load_b.wait}
    for key in list(waits):
        items.append(Item(key, [], (-1.0,), lambda: None))
    items.append(Item(("head",), [("load", 0)], (-0.5,), set_head, takes=0.3))
    single = []

    def send(key, deps, rank, link, source, target, sent, arrives=None, late=0.0):
        if arrives is None:
            arrives = came.at[len(single)]
            single.append(key)
        copy = pltpu.make_async_remote_copy(
            src_ref=source, dst_ref=target, send_sem=sent, recv_sem=arrives,
            device_id=toward[link], device_id_type=MESH,
        )
        if single and single[-1] == key:
            waits[key] = copy.wait_recv
        size = 2 * source.shape[0] * source.shape[1]
        items.append(Item(key, deps, (rank,), copy.start, link, size, late=late))

    arrived = []
    for p in range(parts):
        chunk = GROUPS[p] // 2
        last = []
        for s in range(2):
            head = HEAD if p == 0 and s == 1 else 0
            begin = start[p] + (s if p else 1 - s) * chunk
            here = pl.ds(HEAD - head + begin, head + chunk)
            source = pl.ds(begin, chunk)
            for d in range(2):
                hops = zs // 2 - (s + d) % 2
                for h in range(hops):
                    block = left.at[here, slab(turn(z, h if d else -h, zs))]
                    key = ("a", p, s, d, h)
                    send(
                        key, [("a", p, s, d, h - 1)] if h else [("head",)] if head else [], PACE * min(p, parts - 2) + h + 0.01 * s, f"z{d}",
                        block if h or head else a_hbm.at[source], block, a_sent.at[0],
                        a_came.at[p] if h == hops - 1 else None, 0 if h else FAR_SOURCE,
                    )
                last.append(key)
        key = ("a", p)
        items.append(Item(key, last, (-1.0,), lambda: None))
        size = left.at[pl.ds(0, 4 * chunk + (0 if p else 2 * HEAD)), pl.ds(0, depth)]
        waits[key] = whole(size, a_came.at[p]).wait_recv
        arrived.append([key])

    have = {}
    for i, kind in enumerate(KINDS):
        for b in range(STEPS[kind]):
            rank = 3 * TURN[kind] + 1.5 * b
            have[kind, b] = [("b", kind, b)] + ([("load", 1)] if kind == "own" else [])
            near = []
            for d, (j, h) in enumerate(USES[kind]):
                u = (kind, d, b)
                mine = right_piece(*u, me_north)
                base = [("by", u)] if j else []
                if j:
                    target = b_hbm.at[slab(turn(y, -j, ys)), cols(*u)]
                    link = f"y{h}" if j == 2 else ("y0" if j == 3 else "y1")
                    if j == 2:
                        send(
                            ("far", u), [], rank, link, target, relay.at[h, b], b_sent.at[0],
                            late=FAR_SOURCE,
                        )
                        send(("by", u), [("far", u)], rank, link, relay.at[h, b], mine, b_sent.at[0])
                    else:
                        send(("by", u), [], rank, link, target, mine, b_sent.at[0], late=FAR_SOURCE)
                source = mine if j else b_hbm.at[slab(y), cols(*u)]
                for e in range(2):
                    send(
                        ("bx", u, e, 1), base, rank + (0.0 if e == h else 0.1), f"x{e}",
                        source, mine, b_sent.at[0], late=0 if j else FAR_SOURCE,
                    )
                passed = right_piece(*u, x_at(1 if h else -1))
                send(
                    ("bx", u, h, 2), [("bx", u, h, 1)], rank - 1, f"x{h}",
                    passed, passed, b_sent.at[0],
                )
                have[kind, b] += base + [("bx", u, 0, 1), ("bx", u, 1, 1), ("bx", u, h, 2)]
                for t in range(xs):
                    place = right_piece(*u, x_at(-t))
                    deps = [base, [("bx", u, 0, 1)], [("bx", u, h, 2)], [("bx", u, 1, 1)]][t]
                    send(
                        ("bd", u, t), deps, rank, "core", place if t else source, place,
                        b_sent.at[0], b_came.at[2 * i + b],
                    )
                    near.append(("bd", u, t))
            items.append(Item(("b", kind, b), near, (-1.0,), lambda: None))
            size = right.at[i, pl.ds(0, depth * xs), pl.ds(0, 2 * width(kind))]
            waits["b", kind, b] = whole(size, b_came.at[2 * i + b]).wait_recv

    def multiply(p, kind, b=None):
        across = slice(None) if b is None else slice(b * half, (b + 1) * half)
        return jnp.dot(
            left[HEAD + start[p]:HEAD + start[p] + GROUPS[p], :], right[KINDS.index(kind), :, across],
            preferred_element_type=jnp.float32,
        )

    def scale_in(k, across):
        return code_in[0][k, GROUPS[0]:GROUPS[0] + 1, across].astype(jnp.float32)

    def decode(p, k, across):
        coded = code_in[p][k, :GROUPS[p], across].astype(jnp.float32)
        size = lax.rsqrt(lax.rsqrt(jnp.maximum(jnp.abs(coded), 1e-37)))
        size = size * lax.rsqrt(size)
        return jnp.where(coded < 0, -size, size) * (scale_in(k, across) * (1.0 / TOP))

    def encode(p, k, across, value):
        power = value * gain_out[k, :, across]
        power = power * power
        power = power * power
        power = power * power
        code_out[p][k, :GROUPS[p], across] = jnp.where(value < 0, -power, power).astype(jnp.bfloat16)

    def set_scale(kind, b):
        i = KINDS.index(kind)
        if kind == KINDS[FIRST]:
            if b == 0:
                most = jnp.max(left[:HEAD, :].astype(jnp.float32), axis=0, keepdims=True)
                peak[...] = jnp.broadcast_to(jnp.max(most, axis=1, keepdims=True) * inner, peak.shape)
        for d in range(2):
            first = (2 * b + d) * width(kind)
            across = slice(b * width(kind), (b + 1) * width(kind))
            block = right[i, :, first:first + width(kind)]
            bound = jnp.max(jnp.abs(block.astype(jnp.float32)), axis=0, keepdims=True) * peak[...]
            if kind == "acc":
                bound = bound + scale_in(slot("two", d), across)
            scale = jnp.maximum(bound, 1e-30).astype(jnp.bfloat16)
            gain_out[slot(kind, d), :, across] = TOP / scale.astype(jnp.float32)
            code_out[0][slot(kind, d), GROUPS[0]:, across] = jnp.broadcast_to(scale, (TAIL, width(kind)))

    def slot(kind, d):
        return 2 * KINDS.index(kind) + d

    def part(p, kind, b):
        def run():
            if p == 0:
                set_scale(kind, b)
            value = multiply(p, kind, b)
            for c in range(STEPS[kind]) if b is None else (b,):
                across = slice(c * width(kind), (c + 1) * width(kind))
                for d in range(2):
                    first = (2 * (c if b is None else 0) + d) * width(kind)
                    block = value[:, first:first + width(kind)]
                    if kind == "acc":
                        block = block + decode(p, slot("two", d), across)
                    encode(p, slot(kind, d), across, block)
        return run

    def own(p):
        def run():
            out[start[p]:start[p] + GROUPS[p], :] = multiply(p, "own")
        return run

    def finish(p):
        def run():
            here = slice(start[p], start[p] + GROUPS[p])
            narrow = None
            for h in range(2):
                value = out[here, h * half:(h + 1) * half]
                value = value + decode(p, slot("dir", 1 - h), slice(None)) + decode(p, slot("acc", h), slice(None))
                out[here, h * half:(h + 1) * half] = value
                value = value * value
                for k in range(0, half, LANES):
                    term = value[:, k:k + LANES]
                    narrow = term if narrow is None else narrow + term
            sums_own[:, here] = jnp.sum(narrow.T, axis=0, keepdims=True)
        return run

    def turn_of(p, c):
        return 2 * p + c if p < EARLY else EARLY + p

    for p in range(parts):
        sent_rows = pl.ds(0, GROUPS[p] + (0 if p else TAIL))
        ends = []
        for k, kind in enumerate(KINDS[:3]):
            split = STEPS[kind] == 2 and p < EARLY
            for b in range(2) if split else (None,):
                deps = list(arrived[p])
                for c in range(STEPS[kind]) if b is None else (b,):
                    deps += have[kind, c]
                c = b or 0
                if kind == "acc":
                    deps.append(("two", p, c))
                if p:
                    deps += [("k", 0, kind, e) for e in range(2)]
                if kind != KINDS[FIRST]:
                    deps.append(("k", 0, KINDS[FIRST], 0))
                rank = 3 * p + 4 * k + 0.1 * c
                takes = (MULTIPLY * (0.95 if split else 1.0) + CODE * (0.5 if split else 1.0)) * GROUPS[p] + (0 if p else 0.2)
                items.append(Item(("k", p, kind, c), deps, (rank,), part(p, kind, b), takes=takes))
                across = pl.ds(c * half // 2, half // 2) if split else pl.ds(0, half)
                for d in range(2):
                    i = slot(kind, d)
                    send(
                        ("c", p, kind, c, d), [("k", p, kind, c)], rank, f"y{d}",
                        code_out[p].at[i, sent_rows, across], code_in[p].at[i, sent_rows, across], c_sent.at[p],
                        two_came.at[turn_of(p, c)] if kind == "two" else end_came.at[p],
                    )
                sent = [("c", p, kind, c, d) for d in range(2)]
                if kind == "two":
                    items.append(Item(("two", p, c), sent, (-1.0,), lambda: None))
                    size = code_in[p].at[pl.ds(0, 2), sent_rows, across]
                    waits["two", p, c] = whole(size, two_came.at[turn_of(p, c)]).wait_recv
                else:
                    ends += sent
        deps = arrived[p] + have["own", 0]
        items.append(Item(("own", p), deps, (1000 + p,), own(p), takes=MULTIPLY * GROUPS[p]))
        items.append(Item(("end", p), ends, (-1.0,), lambda: None))
        waits["end", p] = whole(code_in[p].at[pl.ds(2, 4), sent_rows], end_came.at[p]).wait_recv
        deps = [("own", p), ("end", p), ("end", 0)]
        items.append(Item(("fin", p), deps, (500 + p,), finish(p), takes=FINISH * GROUPS[p]))

    shares = ((0, start[LATE]), (start[LATE], rows - start[LATE]))

    farthest = sorted(range(1, n), key=lambda k: abs(k - n // 2))

    def tell(i):
        def run():
            for k in farthest:
                pltpu.make_async_remote_copy(
                    src_ref=sums_own.at[:, pl.ds(*shares[i])], dst_ref=sums_in[i].at[k - 1],
                    send_sem=s_sent.at[i], recv_sem=s_came.at[i],
                    device_id=(me_north, lax.rem(me + k, n)), device_id_type=MESH,
                ).start()
        return run

    early = [("fin", p) for p in range(LATE)]
    items.append(Item(("s", 0), early, (2000,), tell(0), takes=0.3))
    late = [("fin", p) for p in range(LATE, parts)]
    items.append(Item(("s", 1), late + [("s", 0)], (2001,), tell(1), takes=0.3))

    order, _ = plan(items)
    waited = set()
    for item in order:
        for key in item.deps:
            if key in waits and key not in waited:
                waits[key]()
                waited.add(key)
        item.emit()

    piece = 128
    for i, (begin, count) in enumerate(shares):
        whole(sums_in[i], s_came.at[i]).wait_recv()
        total = sums_own[:, pl.ds(begin, count)]
        for k in range(n - 1):
            total = total + sums_in[i][k]
        scale = lax.rsqrt(total / (columns * n) + 1e-06)
        for r in range(0, count, piece):
            gain = jnp.broadcast_to(scale[:, r:r + piece], (LANES, piece)).T
            for k in range(0, columns, LANES):
                out[pl.ds(begin + r, piece), k:k + LANES] *= gain
    whole(left.at[:, pl.ds(0, depth * (zs - 1))], a_sent.at[0]).wait_send()
    whole(right, b_sent.at[0]).wait_send()
    for p in range(parts):
        whole(code_out[p], c_sent.at[p]).wait_send()
    for i in range(2):
        whole(sums_in[i], s_sent.at[i]).wait_send()


def shards(xs, ys, zs, left, right):
    rows, depth = left.shape
    columns = right.shape[1]
    half = columns // 2
    parts = len(GROUPS)
    peers = ys * zs - 1
    dma = pltpu.SemaphoreType.DMA
    codes = [pltpu.VMEM((6, group + (0 if p else TAIL), half), jnp.bfloat16) for p, group in enumerate(GROUPS)]
    pieces = sum(2 * STEPS[kind] for kind in KINDS)
    single = parts * (2 * (zs - 1) - 4) + 3 * pieces + sum(2 * STEPS[kind] for kind in KINDS[:3]) + 2 * STEPS["two"]
    factors = [pltpu.with_memory_space_constraint(v, pltpu.HBM) for v in (left, right)]
    return pl.pallas_call(
        functools.partial(kernel, xs, ys, zs),
        out_shape=jax.ShapeDtypeStruct((rows, columns), jnp.float32),
        in_specs=[pl.BlockSpec(memory_space=pltpu.HBM)] * 2,
        out_specs=pl.BlockSpec(memory_space=pltpu.VMEM),
        scratch_shapes=[
            pltpu.VMEM((HEAD + rows, depth * zs), left.dtype),
            pltpu.VMEM((len(KINDS), depth * 2 * xs, columns), right.dtype),
            pltpu.VMEM((2, STEPS["two"], depth, half // STEPS["two"]), right.dtype),
            pltpu.VMEM((1, rows), jnp.float32),
            *codes,
            *codes,
            pltpu.VMEM((1, half // 2), jnp.float32),
            pltpu.VMEM((6, 1, half), jnp.float32),
            pltpu.VMEM((peers, 1, sum(GROUPS[:LATE])), jnp.float32),
            pltpu.VMEM((peers, 1, sum(GROUPS[LATE:])), jnp.float32),
            dma((2,)),
            dma((1,)),
            dma((1,)),
            dma((parts,)),
            dma((2,)),
            dma((single,)),
            dma((parts,)),
            dma((2 * len(KINDS) - 1,)),
            dma((EARLY + parts,)),
            dma((parts,)),
            dma((2,)),
        ],
        compiler_params=pltpu.CompilerParams(
            collective_id=0, has_side_effects=True, vmem_limit_bytes=40 << 20
        ),
    )(*factors)


def solution(mesh):
    xs = mesh.shape["north"] // 2
    ys = xs
    zs = mesh.shape["east"] // ys
    placed = (P("north", "east"), P("north", "east"))
    return jax.shard_map(
        functools.partial(shards, xs, ys, zs),
        mesh=mesh, in_specs=placed, out_specs=P("north", "east"), check_vma=False,
    )
```
